32 devices in a mesh: cls: 4 (over y, x), row: 8 (over z, core).
Axes of the slice: x: 2, y: 2, z: 4, core: 2. Of those that a mesh axis runs over, the one named last changes fastest.
Arguments:
- binned: int32 [32768, 512], P('row'), may hold values from 0 to 255
- labels: int32 [32768], P('row'), may hold values from 0 to 127
- logits: float32 [32768, 128], P('row', 'cls'), may hold values from -320 to 320
- elected: int32 [128, 12], P('cls'), may hold values from 0 to 511, as said below
- split_slot: int32 [128], P('cls'), may hold values from 0 to 11
- split_bin: int32 [128], P('cls'), may hold values from 0 to 254
Outputs:
- new_logits: float32 [32768, 128], P('row', 'cls')
- split_gains: float32 [128, 12, 256], P(('cls', 'row'))
The draws below stay inside these ranges and needn't reach their ends.
Inputs may be any that keep to these rules, and one draw needn't show every extreme that they name: `elected`: the 12 ids of one class are distinct.
All inputs are finite; a program needn't handle non-finite values.
Results may differ from the reference program's by a relative error of at most 0.002.
Values sent between devices are 32-bit elements; how exact they have to be, the bound alone decides.
A program may use at most 128 MiB of HBM per device.

```python
import jax
import jax.numpy as jnp
from jax import lax

F = 512
B = 256
K = 12
CLASSES = 128
ROWS = 32768


def draw_logits(key, part):
    normal_key = jax.random.fold_in(key, 0)
    scores = 2.0 * jnp.clip(jax.random.normal(normal_key, (ROWS, CLASSES), jnp.float32), -6.0, 6.0)
    return scores


def draw_elected(key, part):
    class_keys = jax.random.split(key, CLASSES)

    def choose_ids(class_key):
        return jax.random.permutation(class_key, F)[:K].astype(jnp.int32)
    return jax.vmap(choose_ids)(class_keys)


def place_ends(array, key, low, high):
    dims = array.shape
    index_at = [jax.random.randint(jax.random.fold_in(key, axis), (), 0, dims[axis]) for axis in range(len(dims))]
    array = array.at[tuple(index_at)].set(low)
    longest = dims.index(max(dims))
    index_at[longest] = (index_at[longest] + 1) % dims[longest]
    return array.at[tuple(index_at)].set(high)


def setup_inputs(seed: int = 0) -> dict:
    keys = jax.random.split(jax.random.key(seed), 7)
    return {
        "binned": place_ends(jax.random.randint(keys[0], (ROWS, F), 0, B), jax.random.fold_in(keys[0], 1), 0, B - 1).astype(jnp.int32),
        "labels": place_ends(jax.random.randint(keys[1], (ROWS,), 0, CLASSES), jax.random.fold_in(keys[1], 1), 0, CLASSES - 1).astype(jnp.int32),
        "logits": draw_logits(jax.random.fold_in(keys[6], 71), 0),
        "elected": draw_elected(jax.random.fold_in(keys[6], 71), 0),
        "split_slot": place_ends(jax.random.randint(keys[4], (CLASSES,), 0, K), jax.random.fold_in(keys[4], 1), 0, K - 1).astype(jnp.int32),
        "split_bin": place_ends(jax.random.randint(keys[5], (CLASSES,), 0, B - 1), jax.random.fold_in(keys[5], 1), 0, (B - 1) - 1).astype(jnp.int32),
    }


reg_lambda = 1.0
step_rate = 0.5


def reference(binned, labels, logits, elected, split_slot, split_bin):
    highest = jnp.max(logits, axis=1, keepdims=True)
    shifted = jnp.exp(logits - highest)
    total = jnp.sum(shifted, axis=1, keepdims=True)
    probs = shifted / total
    class_ids = jnp.arange(CLASSES, dtype=jnp.int32)
    target = (labels[:, None] == class_ids[None, :]).astype(jnp.float32)
    gradient = (probs - target).astype(jnp.bfloat16)
    hessian = (probs * (1.0 - probs)).astype(jnp.bfloat16)

    def per_class(index):
        columns = jnp.take(binned, elected[index], axis=1)
        grad_col = lax.dynamic_slice_in_dim(gradient, index, 1, 1)[:, 0]
        hess_col = lax.dynamic_slice_in_dim(hessian, index, 1, 1)[:, 0]
        weights = jnp.stack([grad_col, hess_col], axis=1).astype(jnp.float32)

        def per_feature(column):
            return jax.ops.segment_sum(weights, column, num_segments=B)

        return jax.vmap(per_feature, in_axes=1)(columns)

    histogram = lax.map(per_class, class_ids)
    histogram = jnp.transpose(histogram, (0, 1, 3, 2))
    running = jnp.cumsum(histogram, axis=-1)
    grad_left = running[:, :, 0, :]
    hess_left = running[:, :, 1, :]
    grad_all = grad_left[:, :, -1:]
    hess_all = hess_left[:, :, -1:]
    split_gains = (grad_left * grad_left / (hess_left + reg_lambda)
                   + (grad_all - grad_left) ** 2 / (hess_all - hess_left + reg_lambda)
                   - grad_all * grad_all / (hess_all + reg_lambda))
    grad_row = jnp.take_along_axis(grad_left, split_slot[:, None, None], axis=1)[:, 0, :]
    hess_row = jnp.take_along_axis(hess_left, split_slot[:, None, None], axis=1)[:, 0, :]
    grad_split = jnp.take_along_axis(grad_row, split_bin[:, None], axis=1)[:, 0]
    hess_split = jnp.take_along_axis(hess_row, split_bin[:, None], axis=1)[:, 0]
    left_leaf = -grad_split / (hess_split + reg_lambda)
    right_leaf = -(grad_row[:, -1] - grad_split) / (hess_row[:, -1] - hess_split + reg_lambda)
    chosen_feature = jnp.take_along_axis(elected, split_slot[:, None], axis=1)[:, 0]
    chosen_bins = jnp.take(binned, chosen_feature, axis=1)
    goes_left = chosen_bins <= split_bin[None, :]
    new_logits = logits + step_rate * jnp.where(goes_left, left_leaf[None, :], right_leaf[None, :])
    return new_logits, split_gains
```

```python
import functools
import math

import jax
import jax.numpy as jnp
from jax import lax
from jax.experimental import pallas as pl
from jax.experimental.pallas import tpu as pltpu
from jax.sharding import PartitionSpec as P

reg_lambda = 1.0
step_rate = 0.5
MESH = pl.DeviceIdType.MESH
NT = (((1,), (1,)), ((), ()))
LOW = 32
HIGH = 8
BINS = LOW * HIGH
UNROLL = 6
BLOCK = 512
LANES = 128
DEPTH = 256
bf16 = jnp.bfloat16
f32 = jnp.float32
narrow = jnp.float8_e4m3fn


def kernel(
    n_cls, n_row, duos, groups_each, unroll, share,
    binned_hbm, x_hbm, labels_hbm, elected_hbm, slot_hbm, split_hbm,
    new_ref, gains_ref,
    binned_ref, x_ref, labels_ref, elected_ref, slot_ref, split_ref,
    meta, picker, low, high, left, grad_ref, hess_ref, grad_rows, hess_rows, stats, sums,
    theirs, mine, first, second,
    load_sem, send_stat, recv_stat, send_sum, recv_sum, send_one, recv_one, send_two, recv_two,
):
    classes, rows = x_ref.shape
    features = elected_ref.shape[0]
    pairs = classes * features
    block = math.gcd(rows, BLOCK)
    blocks = rows // block
    tiles = rows // LANES
    per_block = block // LANES
    cls = lax.axis_index("cls")
    me = lax.axis_index("row")
    core = lax.rem(me, 2)
    chip = me // 2
    chips = n_row // 2
    barrier = pltpu.get_barrier_semaphore()

    def stat_copy(k):
        return pltpu.make_async_remote_copy(
            src_ref=stats.at[0], dst_ref=stats.at[k], send_sem=send_stat.at[k], recv_sem=recv_stat.at[k],
            device_id=(lax.rem(cls + k, n_cls), me), device_id_type=MESH,
        )

    def sum_copy(k):
        return pltpu.make_async_remote_copy(
            src_ref=sums.at[0], dst_ref=sums.at[k], send_sem=send_sum.at[k], recv_sem=recv_sum.at[k],
            device_id=(cls, lax.rem(me + k, n_row)), device_id_type=MESH,
        )

    def one_copy(s):
        return pltpu.make_async_remote_copy(
            src_ref=theirs.at[s], dst_ref=first.at[s], send_sem=send_one.at[s], recv_sem=recv_one.at[s],
            device_id=(cls, 2 * chip + 1 - core), device_id_type=MESH,
        )

    def two_copy(s):
        return pltpu.make_async_remote_copy(
            src_ref=mine.at[s], dst_ref=second.at[s], send_sem=send_two.at[s], recv_sem=recv_two.at[s],
            device_id=(cls, 2 * lax.rem(chip + s + 1, chips) + core), device_id_type=MESH,
        )

    small = [
        pltpu.make_async_copy(src, dst, load_sem.at[blocks + i])
        for i, (src, dst) in enumerate([
            (elected_hbm, elected_ref), (slot_hbm, slot_ref), (split_hbm, split_ref),
            (x_hbm, x_ref), (labels_hbm, labels_ref),
        ])
    ]
    part = [
        pltpu.make_async_copy(
            binned_hbm.at[pl.ds(b * block, block)], binned_ref.at[pl.ds(b * block, block)], load_sem.at[b]
        )
        for b in range(blocks)
    ]

    for k in range(1, n_cls):
        pl.semaphore_signal(barrier, inc=1, device_id=(lax.rem(cls + k, n_cls), me), device_id_type=MESH)
    for k in range(1, n_row):
        pl.semaphore_signal(barrier, inc=1, device_id=(cls, lax.rem(me + k, n_row)), device_id_type=MESH)
    for copy in small[:4]:
        copy.start()
    for copy in part:
        copy.start()
    small[4].start()

    for copy in small[:3]:
        copy.wait()
    meta[...] = jnp.zeros(meta.shape, f32)
    meta[:features, :classes] = elected_ref[...].astype(f32)
    meta[features : features + 1, :classes] = slot_ref[...].astype(f32)
    meta[features + 1 : features + 2, :classes] = split_ref[...].astype(f32)
    turned = meta[...].T
    lane = lax.broadcasted_iota(jnp.int32, (classes, picker.shape[1]), 1).astype(f32)
    slot = turned[:classes, features : features + 1]
    split_column = turned[:classes, features + 1 : features + 2]
    split_feature = jnp.zeros((classes, 1), f32)
    for k in range(features):
        column = turned[:classes, k : k + 1]
        split_feature = jnp.where(slot == k, column, split_feature)
        picker[k * classes : (k + 1) * classes] = (lane == column).astype(f32).astype(bf16)
    picker[pairs:] = (lane == split_feature).astype(f32).astype(bf16)

    small[3].wait()
    for b in range(blocks):
        cols = slice(b * block, (b + 1) * block)
        x = x_ref[:, cols]
        local_max = jnp.max(x, axis=0, keepdims=True)
        stats[0, 0:1, cols] = local_max
        stats[0, 1:2, cols] = jnp.sum(jnp.exp(x - local_max), axis=0, keepdims=True)

    def pick(b):
        part[b].wait()
        here = binned_ref[b * block : (b + 1) * block].astype(f32).astype(bf16)
        picked = lax.dot_general(picker[...], here, NT, preferred_element_type=f32)
        chosen = picked[:pairs]
        top = jnp.floor(chosen * (1.0 / LOW))
        rest = chosen - top * LOW
        for j in range(per_block):
            low[b * per_block + j] = rest[:, j * LANES : (j + 1) * LANES]
            high[b * per_block + j] = top[:, j * LANES : (j + 1) * LANES]
        left[:, b * block : (b + 1) * block] = (picked[pairs:] <= split_column).astype(f32)

    for b in range(blocks // 2):
        pick(b)
    with jax.named_scope("barrier"):
        pl.semaphore_wait(barrier, n_cls - 1 + n_row - 1)
    for k in range(1, n_cls):
        stat_copy(k).start()
    for b in range(blocks // 2, blocks):
        pick(b)

    small[4].wait()
    with jax.named_scope("statwait"):
        for k in range(1, n_cls):
            stat_copy(k).wait()
    class_ids = cls * classes + lax.broadcasted_iota(jnp.int32, (classes, block), 0)
    totals = [jnp.zeros((classes, LANES), f32) for _ in range(4)]
    for b in range(blocks):
        cols = slice(b * block, (b + 1) * block)
        local_max = stats[0, 0:1, cols]
        highest = local_max
        for k in range(1, n_cls):
            highest = jnp.maximum(highest, stats[k, 0:1, cols])
        denom = stats[0, 1:2, cols] * jnp.exp(local_max - highest)
        for k in range(1, n_cls):
            denom = denom + stats[k, 1:2, cols] * jnp.exp(stats[k, 0:1, cols] - highest)
        probs = jnp.exp(x_ref[:, cols] - highest) / denom
        target = (labels_ref[:, cols] == class_ids).astype(f32)
        grad = (probs - target).astype(bf16).astype(f32)
        hess = (probs * (1.0 - probs)).astype(bf16).astype(f32)
        goes = left[:, cols]
        for j in range(per_block):
            at = slice(j * LANES, (j + 1) * LANES)
            grad_ref[b * per_block + j] = grad[:, at]
            hess_ref[b * per_block + j] = hess[:, at]
            for n, term in enumerate((grad * goes, hess * goes, grad, hess)):
                totals[n] = totals[n] + term[:, at]
    spot = lax.broadcasted_iota(jnp.int32, (classes, LANES), 1)
    packed = jnp.zeros((classes, LANES), f32)
    for n in range(4):
        packed = jnp.where(spot == n, jnp.sum(totals[n], axis=1, keepdims=True), packed)
    sums[0] = packed
    for k in range(1, n_row):
        sum_copy(k).start()

    def repeat(c, carry):
        for t in range(tiles):
            g = grad_ref[t, pl.ds(c, 8, stride=0), :]
            h = hess_ref[t, pl.ds(c, 8, stride=0), :]
            grad_rows[c, t] = jnp.concatenate([g, g], axis=0).astype(bf16)
            hess_rows[c, t] = jnp.concatenate([h, h], axis=0).astype(bf16)
        return carry

    with jax.named_scope("repeat"):
        lax.fori_loop(0, classes, repeat, 0)

    sub = lax.broadcasted_iota(jnp.int32, (16, LANES), 0) & (HIGH - 1)
    ids = [(sub + HIGH * n).astype(f32).astype(bf16) for n in range(LOW // HIGH)]
    one = jnp.ones((16, LANES), bf16)
    zero = jnp.zeros((16, LANES), bf16)
    wide = duos * 2 * LOW
    lane_at = lax.broadcasted_iota(jnp.int32, (16, wide), 1)
    lane_pair = lane_at // (2 * LOW) * 2 + lane_at // HIGH % 2
    depth = math.gcd(rows, DEPTH)

    def one_group(dest, g):
        total = None
        for step in range(rows // depth):
            tops = []
            lows = []
            for d in range(duos):
                q = g * duos + d
                c = dest * share + q % share
                p = q // share * 2 * classes + c
                top = [[], []]
                low_rows = [[] for _ in range(LOW // 16)]
                for t in range(step * depth // LANES, (step + 1) * depth // LANES):

                    def both(ref):
                        a = ref[t, pl.ds(p, 8, stride=0), :]
                        b = ref[t, pl.ds(p + classes, 8, stride=0), :]
                        return jnp.concatenate([a, b], axis=0).astype(bf16)

                    lo = both(low)
                    hot = [jnp.where(lo == i, one, zero) for i in ids]
                    for n in range(LOW // 16):
                        low_rows[n].append(jnp.concatenate(hot[2 * n : 2 * n + 2], axis=0).astype(narrow))
                    same = both(high) == ids[0]
                    top[0].append(jnp.where(same, grad_rows[c, t], zero))
                    top[1].append(jnp.where(same, hess_rows[c, t], zero))
                tops += [jnp.concatenate(r, axis=1) for r in top]
                lows += [jnp.concatenate(r, axis=1) for r in low_rows]
            product = lax.dot_general(
                jnp.concatenate(tops, axis=0), jnp.concatenate(lows, axis=0), NT, preferred_element_type=f32
            )
            total = product if total is None else total + product
        kept = None
        for d in range(duos):
            for s in range(2):
                at = d * 32 + s * 8
                piece = jnp.concatenate([total[at : at + 8], total[at + 16 : at + 24]], axis=0)
                kept = piece if kept is None else jnp.where(lane_pair == 2 * d + s, piece, kept)
        return kept

    def fill(target_ref, s, dest):
        def some(i, carry):
            for u in range(unroll):
                target_ref[s, i * unroll + u] = one_group(dest, i * unroll + u)
            return carry

        lax.fori_loop(0, groups_each // unroll, some, 0)

    def each_chip(s, carry):
        dest = lax.rem(chip + s + 1, chips)
        fill(theirs, s, 2 * dest + 1 - core)
        one_copy(s).start()
        fill(mine, s, 2 * dest + core)

        @pl.when(s < chips - 1)
        def _():
            with jax.named_scope("onewait"):
                one_copy(s).wait_recv()
            mine[s] = mine[s] + first[s]
            two_copy(s).start()

        return carry

    with jax.named_scope("hist"):
        lax.fori_loop(0, chips, each_chip, 0)

    total = sums[0]
    with jax.named_scope("sumwait"):
        for k in range(1, n_row):
            sum_copy(k).wait()
    for k in range(1, n_row):
        total = total + sums[k]
    grad_left = total[:, 0:1]
    hess_left = total[:, 1:2]
    left_leaf = -grad_left / (hess_left + reg_lambda)
    right_leaf = -(total[:, 2:3] - grad_left) / (total[:, 3:4] - hess_left + reg_lambda)
    for b in range(blocks):
        cols = slice(b * block, (b + 1) * block)
        new_ref[:, cols] = x_ref[:, cols] + step_rate * jnp.where(left[:, cols] > 0.5, left_leaf, right_leaf)

    with jax.named_scope("tailwait"):
        one_copy(chips - 1).wait_recv()
        for s in range(chips):
            one_copy(s).wait_send()
        for s in range(chips - 1):
            two_copy(s).wait()
    summed = mine[chips - 1] + first[chips - 1]
    for s in range(chips - 1):
        summed = summed + second[s]
    count = groups_each * 2 * HIGH
    here = summed.reshape(count, wide)
    a = lax.broadcasted_iota(jnp.int32, (wide, 2 * wide), 0)
    b = lax.broadcasted_iota(jnp.int32, (wide, 2 * wide), 1)
    duo = a // (2 * LOW)
    pair = (duo // share * 2 + a // HIGH % 2) * share + duo % share
    value = a // (2 * HIGH) % (LOW // HIGH) * HIGH + a % HIGH
    target = b % wide
    keep = (pair == target // LOW) & ((b >= wide) | (value <= target % LOW))
    pieces = []
    rest = here
    for _ in range(3):
        piece = rest.astype(bf16)
        pieces.append(piece)
        rest = rest - piece.astype(f32)
    spread = lax.dot_general(
        jnp.concatenate(pieces, axis=0), keep.astype(f32).astype(bf16), (((1,), (0,)), ((), ())),
        preferred_element_type=f32,
    )
    spread = spread[:count] + spread[count : 2 * count] + spread[2 * count :]
    level = lax.broadcasted_iota(jnp.int32, (HIGH, wide), 0)

    def running(top):
        inside = spread[top : top + HIGH, :wide]
        upto = spread[top : top + HIGH, wide:]
        for shift in (1, 2, 4):
            upto = upto + jnp.where(level >= shift, pltpu.roll(upto, shift, 0), 0.0)
        before = jnp.where(level >= 1, pltpu.roll(upto, 1, 0), 0.0)
        return inside + before, upto[HIGH - 1 :]

    row_at = lax.broadcasted_iota(jnp.int32, (HIGH, BINS), 0)
    block_at = lax.broadcasted_iota(jnp.int32, (HIGH, BINS), 1) // LOW
    for g in range(groups_each):
        gl, ga = running(g * 2 * HIGH)
        hl, ha = running(g * 2 * HIGH + HIGH)
        gains = (
            gl * gl / (hl + reg_lambda)
            + (ga - gl) * (ga - gl) / (ha - hl + reg_lambda)
            - ga * ga / (ha + reg_lambda)
        )
        if wide < BINS:
            gains = jnp.concatenate([gains, jnp.zeros((HIGH, BINS - wide), f32)], axis=1)
        turned = gains
        for d in range(1, HIGH):
            moved = pltpu.roll(pltpu.roll(gains, HIGH - d, 0), LOW * d, 1)
            turned = jnp.where((row_at + d) % HIGH == block_at, moved, turned)
        each = 2 * duos // share
        for k in range(each):
            gains_ref[g * each + k] = turned[k * share : (k + 1) * share]


def local(n_cls, n_row, binned, labels, logits, elected, split_slot, split_bin):
    rows, classes = logits.shape
    columns = binned.shape[1]
    features = elected.shape[1]
    pairs = classes * features
    share = classes // n_row
    duos = math.gcd(share * features // 2, 4)
    groups_each = share * features // 2 // duos
    unroll = math.gcd(groups_each, UNROLL)
    chips = n_row // 2
    blocks = rows // math.gcd(rows, BLOCK)
    tiles = rows // LANES
    dma = pltpu.SemaphoreType.DMA
    part = (chips, groups_each, 2 * HIGH, duos * 2 * LOW)
    anywhere = pl.BlockSpec(memory_space=pltpu.HBM)
    vmem = pltpu.VMEM

    new, gains = pl.pallas_call(
        functools.partial(kernel, n_cls, n_row, duos, groups_each, unroll, share),
        out_shape=[jax.ShapeDtypeStruct((classes, rows), f32), jax.ShapeDtypeStruct((features, share, BINS), f32)],
        in_specs=[anywhere] * 6,
        out_specs=[pl.BlockSpec(memory_space=pltpu.VMEM)] * 2,
        scratch_shapes=[
            vmem((rows, columns), jnp.int32), vmem((classes, rows), f32), vmem((1, rows), jnp.int32),
            vmem((features, classes), jnp.int32), vmem((1, classes), jnp.int32), vmem((1, classes), jnp.int32),
            vmem((128, 128), f32),
            vmem((pairs + classes, columns), bf16),
            vmem((tiles, pairs, LANES), f32), vmem((tiles, pairs, LANES), f32),
            vmem((classes, rows), f32),
            vmem((tiles, classes, LANES), f32), vmem((tiles, classes, LANES), f32),
            vmem((classes, tiles, 16, LANES), bf16), vmem((classes, tiles, 16, LANES), bf16),
            vmem((n_cls, 2, rows), f32),
            vmem((n_row, classes, LANES), f32),
            vmem(part, f32), vmem(part, f32), vmem(part, f32), vmem(part, f32),
            dma((blocks + 5,)), dma((n_cls,)), dma((n_cls,)), dma((n_row,)), dma((n_row,)),
            dma((chips,)), dma((chips,)), dma((chips,)), dma((chips,)),
        ],
        compiler_params=pltpu.CompilerParams(
            vmem_limit_bytes=52 * 1024 * 1024, collective_id=0, has_side_effects=True,
        ),
        name="round",
    )(
        *[pltpu.with_memory_space_constraint(array, pltpu.HBM) for array in (
            binned, logits.T, labels.reshape(1, rows), elected.T,
            split_slot.reshape(1, classes), split_bin.reshape(1, classes),
        )]
    )
    return new.T, gains.transpose(1, 0, 2)


def solution(mesh):
    return jax.shard_map(
        functools.partial(local, mesh.shape["cls"], mesh.shape["row"]),
        mesh=mesh,
        in_specs=(P("row", None), P("row"), P("row", "cls"), P("cls", None), P("cls"), P("cls")),
        out_specs=(P("row", "cls"), P(("cls", "row"), None, None)),
        check_vma=False,
    )
```

```python
import functools
import math

import jax
import jax.numpy as jnp
from jax import lax
from jax.experimental import pallas as pl
from jax.experimental.pallas import tpu as pltpu
from jax.sharding import PartitionSpec as P

reg_lambda = 1.0
step_rate = 0.5
MESH = pl.DeviceIdType.MESH
NT = (((1,), (1,)), ((), ()))
LOW = 32
HIGH = 8
BINS = LOW * HIGH
UNROLL = 6
BLOCK = 512
LANES = 128
DEPTH = 256
bf16 = jnp.bfloat16
f32 = jnp.float32
narrow = jnp.float8_e4m3fn


def prepare(
    n_cls,
    binned_hbm, x_hbm, labels_hbm, elected_hbm, slot_hbm, split_hbm,
    low, high, left, grad_rows, hess_rows, sums_ref,
    binned_ref, x_ref, labels_ref, elected_ref, slot_ref, split_ref,
    meta, picker, grad_ref, hess_ref, stats,
    load_sem, send_stat, recv_stat,
):
    classes, rows = x_ref.shape
    features = elected_ref.shape[0]
    pairs = classes * features
    block = math.gcd(rows, BLOCK)
    blocks = rows // block
    tiles = rows // LANES
    per_block = block // LANES
    cls = lax.axis_index("cls")
    me = lax.axis_index("row")
    barrier = pltpu.get_barrier_semaphore()

    def stat_copy(k):
        return pltpu.make_async_remote_copy(
            src_ref=stats.at[0], dst_ref=stats.at[k], send_sem=send_stat.at[k], recv_sem=recv_stat.at[k],
            device_id=(lax.rem(cls + k, n_cls), me), device_id_type=MESH,
        )

    small = [
        pltpu.make_async_copy(src, dst, load_sem.at[blocks + i])
        for i, (src, dst) in enumerate([
            (elected_hbm, elected_ref), (slot_hbm, slot_ref), (split_hbm, split_ref),
            (x_hbm, x_ref), (labels_hbm, labels_ref),
        ])
    ]
    part = [
        pltpu.make_async_copy(
            binned_hbm.at[pl.ds(b * block, block)], binned_ref.at[pl.ds(b * block, block)], load_sem.at[b]
        )
        for b in range(blocks)
    ]

    for k in range(1, n_cls):
        pl.semaphore_signal(barrier, inc=1, device_id=(lax.rem(cls + k, n_cls), me), device_id_type=MESH)
    for copy in small[:4]:
        copy.start()
    for copy in part:
        copy.start()
    small[4].start()

    for copy in small[:3]:
        copy.wait()
    meta[...] = jnp.zeros(meta.shape, f32)
    meta[:features, :classes] = elected_ref[...].astype(f32)
    meta[features : features + 1, :classes] = slot_ref[...].astype(f32)
    meta[features + 1 : features + 2, :classes] = split_ref[...].astype(f32)
    turned = meta[...].T
    lane = lax.broadcasted_iota(jnp.int32, (classes, picker.shape[1]), 1).astype(f32)
    slot = turned[:classes, features : features + 1]
    split_column = turned[:classes, features + 1 : features + 2]
    split_feature = jnp.zeros((classes, 1), f32)
    for k in range(features):
        column = turned[:classes, k : k + 1]
        split_feature = jnp.where(slot == k, column, split_feature)
        picker[k * classes : (k + 1) * classes] = (lane == column).astype(f32).astype(bf16)
    picker[pairs:] = (lane == split_feature).astype(f32).astype(bf16)

    small[3].wait()
    for b in range(blocks):
        cols = slice(b * block, (b + 1) * block)
        x = x_ref[:, cols]
        local_max = jnp.max(x, axis=0, keepdims=True)
        stats[0, 0:1, cols] = local_max
        stats[0, 1:2, cols] = jnp.sum(jnp.exp(x - local_max), axis=0, keepdims=True)

    def pick(b):
        part[b].wait()
        here = binned_ref[b * block : (b + 1) * block].astype(f32).astype(bf16)
        picked = lax.dot_general(picker[...], here, NT, preferred_element_type=f32)
        chosen = picked[:pairs]
        top = jnp.floor(chosen * (1.0 / LOW))
        rest = chosen - top * LOW
        for j in range(per_block):
            low[b * per_block + j] = rest[:, j * LANES : (j + 1) * LANES]
            high[b * per_block + j] = top[:, j * LANES : (j + 1) * LANES]
        left[:, b * block : (b + 1) * block] = (picked[pairs:] <= split_column).astype(f32)

    with jax.named_scope("barrier"):
        pl.semaphore_wait(barrier, n_cls - 1)
    for k in range(1, n_cls):
        stat_copy(k).start()
    for b in range(blocks):
        pick(b)

    small[4].wait()
    with jax.named_scope("statwait"):
        for k in range(1, n_cls):
            stat_copy(k).wait()
    class_ids = cls * classes + lax.broadcasted_iota(jnp.int32, (classes, block), 0)
    totals = [jnp.zeros((classes, LANES), f32) for _ in range(4)]
    for b in range(blocks):
        cols = slice(b * block, (b + 1) * block)
        local_max = stats[0, 0:1, cols]
        highest = local_max
        for k in range(1, n_cls):
            highest = jnp.maximum(highest, stats[k, 0:1, cols])
        denom = stats[0, 1:2, cols] * jnp.exp(local_max - highest)
        for k in range(1, n_cls):
            denom = denom + stats[k, 1:2, cols] * jnp.exp(stats[k, 0:1, cols] - highest)
        probs = jnp.exp(x_ref[:, cols] - highest) / denom
        target = (labels_ref[:, cols] == class_ids).astype(f32)
        grad = (probs - target).astype(bf16).astype(f32)
        hess = (probs * (1.0 - probs)).astype(bf16).astype(f32)
        goes = left[:, cols]
        for j in range(per_block):
            at = slice(j * LANES, (j + 1) * LANES)
            grad_ref[b * per_block + j] = grad[:, at]
            hess_ref[b * per_block + j] = hess[:, at]
            for n, term in enumerate((grad * goes, hess * goes, grad, hess)):
                totals[n] = totals[n] + term[:, at]
    spot = lax.broadcasted_iota(jnp.int32, (classes, LANES), 1)
    packed = jnp.zeros((classes, LANES), f32)
    for n in range(4):
        packed = jnp.where(spot == n, jnp.sum(totals[n], axis=1, keepdims=True), packed)
    sums_ref[...] = packed

    def repeat(c, carry):
        for t in range(tiles):
            g = grad_ref[t, pl.ds(c, 8, stride=0), :]
            h = hess_ref[t, pl.ds(c, 8, stride=0), :]
            grad_rows[c, t] = jnp.concatenate([g, g], axis=0).astype(bf16)
            hess_rows[c, t] = jnp.concatenate([h, h], axis=0).astype(bf16)
        return carry

    with jax.named_scope("repeat"):
        lax.fori_loop(0, classes, repeat, 0)


def reduce(
    n_row, duos, groups_each, unroll, share, features,
    x_hbm, low, high, left, grad_rows, hess_rows, sums_ref,
    new_ref, gains_ref,
    x_ref, sums, work, first, second,
    load_sem, send_sum, recv_sum, send_one, recv_one, send_two, recv_two,
):
    classes, rows = x_ref.shape
    block = math.gcd(rows, BLOCK)
    blocks = rows // block
    cls = lax.axis_index("cls")
    me = lax.axis_index("row")
    core = lax.rem(me, 2)
    chip = me // 2
    chips = n_row // 2
    barrier = pltpu.get_barrier_semaphore()

    def sum_copy(k):
        return pltpu.make_async_remote_copy(
            src_ref=sums.at[0], dst_ref=sums.at[k], send_sem=send_sum.at[k], recv_sem=recv_sum.at[k],
            device_id=(cls, lax.rem(me + k, n_row)), device_id_type=MESH,
        )

    def one_copy(s):
        return pltpu.make_async_remote_copy(
            src_ref=work.at[2 * s], dst_ref=first.at[s], send_sem=send_one.at[s], recv_sem=recv_one.at[s],
            device_id=(cls, 2 * chip + 1 - core), device_id_type=MESH,
        )

    def two_copy(s):
        return pltpu.make_async_remote_copy(
            src_ref=work.at[2 * s + 1], dst_ref=second.at[s], send_sem=send_two.at[s], recv_sem=recv_two.at[s],
            device_id=(cls, 2 * lax.rem(chip + s + 1, chips) + core), device_id_type=MESH,
        )

    for k in range(1, n_row):
        pl.semaphore_signal(barrier, inc=1, device_id=(cls, lax.rem(me + k, n_row)), device_id_type=MESH)
    load = pltpu.make_async_copy(x_hbm, x_ref, load_sem.at[0])
    load.start()
    sums[0] = sums_ref[...]

    sub = lax.broadcasted_iota(jnp.int32, (16, LANES), 0) & (HIGH - 1)
    ids = [(sub + HIGH * n).astype(f32).astype(bf16) for n in range(LOW // HIGH)]
    one = jnp.ones((16, LANES), bf16)
    zero = jnp.zeros((16, LANES), bf16)
    wide = duos * 2 * LOW
    lane_at = lax.broadcasted_iota(jnp.int32, (16, wide), 1)
    lane_pair = lane_at // (2 * LOW) * 2 + lane_at // HIGH % 2
    depth = math.gcd(rows, DEPTH)

    def one_group(dest, g):
        total = None
        for step in range(rows // depth):
            tops = []
            lows = []
            for d in range(duos):
                c = dest * share + d % share
                p = g * (duos // share * 2 * classes) + dest * share + (d // share * 2 * classes + d % share)
                top = [[], []]
                hot = [[] for _ in ids]
                for t in range(step * depth // LANES, (step + 1) * depth // LANES):

                    def both(ref):
                        a = ref[t, pl.ds(p, 8, stride=0), :]
                        b = ref[t, pl.ds(p + classes, 8, stride=0), :]
                        return jnp.concatenate([a, b], axis=0).astype(bf16)

                    lo = both(low)
                    hi = both(high)
                    g_row = grad_rows[c, t]
                    h_row = hess_rows[c, t]
                    for n, i in enumerate(ids):
                        hot[n].append(jnp.where(lo == i, one, zero))
                    same = hi == ids[0]
                    top[0].append(jnp.where(same, g_row, zero))
                    top[1].append(jnp.where(same, h_row, zero))
                for n in range(0, len(ids), 2):
                    lows.append(jnp.concatenate([
                        jnp.concatenate(pair, axis=0).astype(narrow) for pair in zip(hot[n], hot[n + 1])
                    ], axis=1))
                tops += [jnp.concatenate(r, axis=1) for r in top]
            product = lax.dot_general(
                jnp.concatenate(tops, axis=0), jnp.concatenate(lows, axis=0), NT, preferred_element_type=f32
            )
            total = product if total is None else total + product
        kept = None
        for d in range(duos):
            for s in range(2):
                at = d * 32 + s * 8
                piece = jnp.concatenate([total[at : at + 8], total[at + 16 : at + 24]], axis=0)
                kept = piece if kept is None else jnp.where(lane_pair == 2 * d + s, piece, kept)
        return kept

    def each_dest(j, carry):
        def some(i, inner):
            for u in range(unroll):
                at = (j * groups_each) + i * unroll + u
                k = at // groups_each
                dest = 2 * lax.rem(chip + k // 2 + 1, chips) + lax.rem(core + 1 + lax.rem(k, 2), 2)
                g = lax.rem(at, groups_each)
                work[k, g] = one_group(dest, g)
            return inner

        lax.fori_loop(0, groups_each // unroll, some, 0)
        s = j // 2
        own = lax.rem(j, 2)

        def pass_on(n):
            one_copy(n).wait_recv()
            work[2 * n + 1] = work[2 * n + 1] + first[n]
            two_copy(n).start()

        @pl.when(j == 1)
        def _():
            with jax.named_scope("rowbarrier"):
                pl.semaphore_wait(barrier, n_row - 1)
            for k in range(1, n_row):
                sum_copy(k).start()
            one_copy(0).start()

        @pl.when((own == 0) & (j > 1))
        def _():
            one_copy(s).start()

        @pl.when(j == 3)
        def _():
            pass_on(0)

        @pl.when((own == 1) & (s > 0) & (s < chips - 1))
        def _():
            pass_on(s)

        return carry

    with jax.named_scope("hist"):
        lax.fori_loop(0, 2 * chips, each_dest, 0)

    load.wait()
    total = sums[0]
    with jax.named_scope("sumwait"):
        for k in range(1, n_row):
            sum_copy(k).wait()
    for k in range(1, n_row):
        total = total + sums[k]
    grad_left = total[:, 0:1]
    hess_left = total[:, 1:2]
    left_leaf = -grad_left / (hess_left + reg_lambda)
    right_leaf = -(total[:, 2:3] - grad_left) / (total[:, 3:4] - hess_left + reg_lambda)
    for b in range(blocks):
        cols = slice(b * block, (b + 1) * block)
        new_ref[:, cols] = x_ref[:, cols] + step_rate * jnp.where(left[:, cols] > 0.5, left_leaf, right_leaf)

    with jax.named_scope("tailwait"):
        one_copy(chips - 1).wait_recv()
        for s in range(chips):
            one_copy(s).wait_send()
        for s in range(chips - 1):
            two_copy(s).wait()
    summed = work[2 * chips - 1] + first[chips - 1]
    for s in range(chips - 1):
        summed = summed + second[s]
    count = groups_each * 2 * HIGH
    here = summed.reshape(count, wide)
    a = lax.broadcasted_iota(jnp.int32, (wide, 2 * wide), 0)
    b = lax.broadcasted_iota(jnp.int32, (wide, 2 * wide), 1)
    duo = a // (2 * LOW)
    pair = (duo // share * 2 + a // HIGH % 2) * share + duo % share
    value = a // (2 * HIGH) % (LOW // HIGH) * HIGH + a % HIGH
    target = b % wide
    keep = (pair == target // LOW) & ((b >= wide) | (value <= target % LOW))
    pieces = []
    rest = here
    for _ in range(3):
        piece = rest.astype(bf16)
        pieces.append(piece)
        rest = rest - piece.astype(f32)
    spread = lax.dot_general(
        jnp.concatenate(pieces, axis=0), keep.astype(f32).astype(bf16), (((1,), (0,)), ((), ())),
        preferred_element_type=f32,
    )
    spread = spread[:count] + spread[count : 2 * count] + spread[2 * count :]
    level = lax.broadcasted_iota(jnp.int32, (HIGH, wide), 0)

    def running(top):
        inside = spread[top : top + HIGH, :wide]
        upto = spread[top : top + HIGH, wide:]
        for shift in (1, 2, 4):
            upto = upto + jnp.where(level >= shift, pltpu.roll(upto, shift, 0), 0.0)
        before = jnp.where(level >= 1, pltpu.roll(upto, 1, 0), 0.0)
        return inside + before, upto[HIGH - 1 :]

    row_at = lax.broadcasted_iota(jnp.int32, (HIGH, BINS), 0)
    block_at = lax.broadcasted_iota(jnp.int32, (HIGH, BINS), 1) // LOW
    for g in range(groups_each):
        gl, ga = running(g * 2 * HIGH)
        hl, ha = running(g * 2 * HIGH + HIGH)
        gains = (
            gl * gl / (hl + reg_lambda)
            + (ga - gl) * (ga - gl) / (ha - hl + reg_lambda)
            - ga * ga / (ha + reg_lambda)
        )
        if wide < BINS:
            gains = jnp.concatenate([gains, jnp.zeros((HIGH, BINS - wide), f32)], axis=1)
        turned = gains
        for d in range(1, HIGH):
            moved = pltpu.roll(pltpu.roll(gains, HIGH - d, 0), LOW * d, 1)
            turned = jnp.where((row_at + d) % HIGH == block_at, moved, turned)
        each = 2 * duos // share
        for k in range(each):
            gains_ref[g * each + k] = turned[k * share : (k + 1) * share]


def deliver(new_ref, gains_ref, new_hbm, gains_hbm, sem):
    copies = [
        pltpu.make_async_copy(new_ref, new_hbm, sem.at[0]),
        pltpu.make_async_copy(gains_ref, gains_hbm, sem.at[1]),
    ]
    for copy in copies:
        copy.start()
    for copy in copies:
        copy.wait()


def local(n_cls, n_row, binned, labels, logits, elected, split_slot, split_bin):
    rows, classes = logits.shape
    columns = binned.shape[1]
    features = elected.shape[1]
    pairs = classes * features
    share = classes // n_row
    duos = math.gcd(share * features // 2, 4)
    groups_each = share * features // 2 // duos
    unroll = math.gcd(groups_each, UNROLL)
    chips = n_row // 2
    blocks = rows // math.gcd(rows, BLOCK)
    tiles = rows // LANES
    dma = pltpu.SemaphoreType.DMA
    part = (chips, groups_each, 2 * HIGH, duos * 2 * LOW)
    anywhere = pl.BlockSpec(memory_space=pltpu.HBM)
    vmem = pltpu.VMEM

    inside = pl.BlockSpec(memory_space=pltpu.VMEM)
    logits_t = pltpu.with_memory_space_constraint(logits.T, pltpu.HBM)
    made = pl.pallas_call(
        functools.partial(prepare, n_cls),
        out_shape=[
            jax.ShapeDtypeStruct((tiles, pairs, LANES), f32), jax.ShapeDtypeStruct((tiles, pairs, LANES), f32),
            jax.ShapeDtypeStruct((classes, rows), f32),
            jax.ShapeDtypeStruct((classes, tiles, 16, LANES), bf16),
            jax.ShapeDtypeStruct((classes, tiles, 16, LANES), bf16),
            jax.ShapeDtypeStruct((classes, LANES), f32),
        ],
        in_specs=[anywhere] * 6,
        out_specs=[inside] * 6,
        scratch_shapes=[
            vmem((rows, columns), jnp.int32), vmem((classes, rows), f32), vmem((1, rows), jnp.int32),
            vmem((features, classes), jnp.int32), vmem((1, classes), jnp.int32), vmem((1, classes), jnp.int32),
            vmem((128, 128), f32),
            vmem((pairs + classes, columns), bf16),
            vmem((tiles, classes, LANES), f32), vmem((tiles, classes, LANES), f32),
            vmem((n_cls, 2, rows), f32),
            dma((blocks + 5,)), dma((n_cls,)), dma((n_cls,)),
        ],
        compiler_params=pltpu.CompilerParams(
            vmem_limit_bytes=24 * 1024 * 1024, collective_id=0, has_side_effects=True,
        ),
        name="prepare",
    )(
        pltpu.with_memory_space_constraint(binned, pltpu.HBM), logits_t,
        *[pltpu.with_memory_space_constraint(array, pltpu.HBM) for array in (
            labels.reshape(1, rows), elected.T, split_slot.reshape(1, classes), split_bin.reshape(1, classes),
        )]
    )
    new, gains = pl.pallas_call(
        functools.partial(reduce, n_row, duos, groups_each, unroll, share, features),
        out_shape=[
            jax.ShapeDtypeStruct((classes, rows), f32), jax.ShapeDtypeStruct((features, share, BINS), f32),
        ],
        in_specs=[anywhere] + [inside] * 6,
        out_specs=[inside] * 2,
        scratch_shapes=[
            vmem((classes, rows), f32), vmem((n_row, classes, LANES), f32),
            vmem((2 * chips, *part[1:]), f32), vmem(part, f32), vmem(part, f32),
            dma((1,)), dma((n_row,)), dma((n_row,)),
            dma((chips,)), dma((chips,)), dma((chips,)), dma((chips,)),
        ],
        compiler_params=pltpu.CompilerParams(
            vmem_limit_bytes=24 * 1024 * 1024, collective_id=1, has_side_effects=True,
        ),
        name="reduce",
    )(logits_t, *[pltpu.with_memory_space_constraint(array, pltpu.VMEM) for array in made])
    new, gains = pl.pallas_call(
        deliver,
        out_shape=[jax.ShapeDtypeStruct(new.shape, f32), jax.ShapeDtypeStruct(gains.shape, f32)],
        in_specs=[inside] * 2,
        out_specs=[pl.BlockSpec(memory_space=pltpu.HBM)] * 2,
        scratch_shapes=[dma((2,))],
        name="deliver",
    )(*[pltpu.with_memory_space_constraint(array, pltpu.VMEM) for array in (new, gains)])
    return new.T, gains.transpose(1, 0, 2)


def solution(mesh):
    return jax.shard_map(
        functools.partial(local, mesh.shape["cls"], mesh.shape["row"]),
        mesh=mesh,
        in_specs=(P("row", None), P("row"), P("row", "cls"), P("cls", None), P("cls"), P("cls")),
        out_specs=(P("row", "cls"), P(("cls", "row"), None, None)),
        check_vma=False,
    )
```

```python
import functools
import math

import jax
import jax.numpy as jnp
from jax import lax
from jax.experimental import pallas as pl
from jax.experimental.pallas import tpu as pltpu
from jax.sharding import PartitionSpec as P

reg_lambda = 1.0
step_rate = 0.5
MESH = pl.DeviceIdType.MESH
NT = (((1,), (1,)), ((), ()))
LOW = 32
HIGH = 8
BINS = LOW * HIGH
UNROLL = 6
BLOCK = 512
LANES = 128
DEPTH = 256
bf16 = jnp.bfloat16
f32 = jnp.float32
narrow = jnp.float8_e4m3fn


def prepare(
    n_cls,
    binned_hbm, x_hbm, labels_hbm, elected_hbm, slot_hbm, split_hbm,
    low, high, left, grad_rows, hess_rows, sums_ref,
    binned_ref, x_ref, labels_ref, elected_ref, slot_ref, split_ref,
    meta, picker, grad_ref, hess_ref, stats,
    load_sem, send_stat, recv_stat,
):
    classes, rows = x_ref.shape
    features = elected_ref.shape[0]
    pairs = classes * features
    block = math.gcd(rows, BLOCK)
    blocks = rows // block
    tiles = rows // LANES
    per_block = block // LANES
    cls = lax.axis_index("cls")
    me = lax.axis_index("row")
    barrier = pltpu.get_barrier_semaphore()

    halves = stats.shape[0]
    per_half = blocks // halves

    def stat_copy(h, k):
        return pltpu.make_async_remote_copy(
            src_ref=stats.at[h, 0], dst_ref=stats.at[h, k],
            send_sem=send_stat.at[h, k], recv_sem=recv_stat.at[h, k],
            device_id=(lax.rem(cls + k, n_cls), me), device_id_type=MESH,
        )

    small = [
        pltpu.make_async_copy(src, dst, load_sem.at[blocks + i])
        for i, (src, dst) in enumerate([
            (elected_hbm, elected_ref), (slot_hbm, slot_ref), (split_hbm, split_ref),
            (x_hbm, x_ref), (labels_hbm, labels_ref),
        ])
    ]
    part = [
        pltpu.make_async_copy(
            binned_hbm.at[pl.ds(b * block, block)], binned_ref.at[pl.ds(b * block, block)], load_sem.at[b]
        )
        for b in range(blocks)
    ]

    for k in range(1, n_cls):
        pl.semaphore_signal(barrier, inc=1, device_id=(lax.rem(cls + k, n_cls), me), device_id_type=MESH)
    for copy in small[:4]:
        copy.start()
    for copy in part:
        copy.start()
    small[4].start()

    for copy in small[:3]:
        copy.wait()
    meta[...] = jnp.zeros(meta.shape, f32)
    meta[:features, :classes] = elected_ref[...].astype(f32)
    meta[features : features + 1, :classes] = slot_ref[...].astype(f32)
    meta[features + 1 : features + 2, :classes] = split_ref[...].astype(f32)
    turned = meta[...].T
    lane = lax.broadcasted_iota(jnp.int32, (classes, picker.shape[1]), 1).astype(f32)
    slot = turned[:classes, features : features + 1]
    split_column = turned[:classes, features + 1 : features + 2]
    split_feature = jnp.zeros((classes, 1), f32)
    for k in range(features):
        column = turned[:classes, k : k + 1]
        split_feature = jnp.where(slot == k, column, split_feature)
        picker[k * classes : (k + 1) * classes] = (lane == column).astype(f32).astype(bf16)
    picker[pairs:] = (lane == split_feature).astype(f32).astype(bf16)

    small[3].wait()
    for b in range(blocks):
        cols = slice(b * block, (b + 1) * block)
        x = x_ref[:, cols]
        local_max = jnp.max(x, axis=0, keepdims=True)
        half = slice(b % per_half * block, (b % per_half + 1) * block)
        stats[b // per_half, 0, 0:1, half] = local_max
        stats[b // per_half, 0, 1:2, half] = jnp.sum(jnp.exp(x - local_max), axis=0, keepdims=True)

    def pick(b):
        part[b].wait()
        here = binned_ref[b * block : (b + 1) * block].astype(f32).astype(bf16)
        picked = lax.dot_general(picker[...], here, NT, preferred_element_type=f32)
        chosen = picked[:pairs]
        top = jnp.floor(chosen * (1.0 / LOW))
        rest = chosen - top * LOW
        for j in range(per_block):
            low[b * per_block + j] = rest[:, j * LANES : (j + 1) * LANES]
            high[b * per_block + j] = top[:, j * LANES : (j + 1) * LANES]
        left[:, b * block : (b + 1) * block] = (picked[pairs:] <= split_column).astype(f32)

    with jax.named_scope("barrier"):
        pl.semaphore_wait(barrier, n_cls - 1)
    for h in range(halves):
        for k in range(1, n_cls):
            stat_copy(h, k).start()
    for b in range(blocks):
        pick(b)

    small[4].wait()
    class_ids = cls * classes + lax.broadcasted_iota(jnp.int32, (classes, block), 0)
    totals = [jnp.zeros((classes, LANES), f32) for _ in range(4)]
    for b in range(blocks):
        cols = slice(b * block, (b + 1) * block)
        h = b // per_half
        if b % per_half == 0:
            for k in range(1, n_cls):
                stat_copy(h, k).wait()
        half = slice(b % per_half * block, (b % per_half + 1) * block)
        local_max = stats[h, 0, 0:1, half]
        highest = local_max
        for k in range(1, n_cls):
            highest = jnp.maximum(highest, stats[h, k, 0:1, half])
        denom = stats[h, 0, 1:2, half] * jnp.exp(local_max - highest)
        for k in range(1, n_cls):
            denom = denom + stats[h, k, 1:2, half] * jnp.exp(stats[h, k, 0:1, half] - highest)
        probs = jnp.exp(x_ref[:, cols] - highest) / denom
        target = (labels_ref[:, cols] == class_ids).astype(f32)
        grad = (probs - target).astype(bf16).astype(f32)
        hess = (probs * (1.0 - probs)).astype(bf16).astype(f32)
        goes = left[:, cols]
        for j in range(per_block):
            at = slice(j * LANES, (j + 1) * LANES)
            grad_ref[b * per_block + j] = grad[:, at]
            hess_ref[b * per_block + j] = hess[:, at]
            for n, term in enumerate((grad * goes, hess * goes, grad, hess)):
                totals[n] = totals[n] + term[:, at]
    spot = lax.broadcasted_iota(jnp.int32, (classes, LANES), 1)
    packed = jnp.zeros((classes, LANES), f32)
    for n in range(4):
        packed = jnp.where(spot == n, jnp.sum(totals[n], axis=1, keepdims=True), packed)
    sums_ref[...] = packed

    def repeat(c, carry):
        for t in range(tiles):
            g = grad_ref[t, pl.ds(c, 8, stride=0), :]
            h = hess_ref[t, pl.ds(c, 8, stride=0), :]
            grad_rows[c, t] = jnp.concatenate([g, g], axis=0).astype(bf16)
            hess_rows[c, t] = jnp.concatenate([h, h], axis=0).astype(bf16)
        return carry

    with jax.named_scope("repeat"):
        lax.fori_loop(0, classes, repeat, 0)


def reduce(
    n_row, duos, groups_each, unroll, share, features,
    x_hbm, low, high, left, grad_rows, hess_rows, sums_ref,
    new_ref, gains_ref,
    x_ref, sums, work, first, second,
    load_sem, send_sum, recv_sum, send_one, recv_one, send_two, recv_two,
):
    classes, rows = x_ref.shape
    block = math.gcd(rows, BLOCK)
    blocks = rows // block
    cls = lax.axis_index("cls")
    me = lax.axis_index("row")
    core = lax.rem(me, 2)
    chip = me // 2
    chips = n_row // 2
    barrier = pltpu.get_barrier_semaphore()

    def sum_copy(k):
        return pltpu.make_async_remote_copy(
            src_ref=sums.at[0], dst_ref=sums.at[k], send_sem=send_sum.at[k], recv_sem=recv_sum.at[k],
            device_id=(cls, lax.rem(me + k, n_row)), device_id_type=MESH,
        )

    def one_copy(s):
        return pltpu.make_async_remote_copy(
            src_ref=work.at[2 * s], dst_ref=first.at[s], send_sem=send_one.at[s], recv_sem=recv_one.at[s],
            device_id=(cls, 2 * chip + 1 - core), device_id_type=MESH,
        )

    def two_copy(s):
        return pltpu.make_async_remote_copy(
            src_ref=work.at[2 * s + 1], dst_ref=second.at[s], send_sem=send_two.at[s], recv_sem=recv_two.at[s],
            device_id=(cls, 2 * lax.rem(chip + s + 1, chips) + core), device_id_type=MESH,
        )

    for k in range(1, n_row):
        pl.semaphore_signal(barrier, inc=1, device_id=(cls, lax.rem(me + k, n_row)), device_id_type=MESH)
    load = pltpu.make_async_copy(x_hbm, x_ref, load_sem.at[0])
    load.start()
    sums[0] = sums_ref[...]

    sub = lax.broadcasted_iota(jnp.int32, (16, LANES), 0) & (HIGH - 1)
    ids = [(sub + HIGH * n).astype(f32).astype(bf16) for n in range(LOW // HIGH)]
    one = jnp.ones((16, LANES), bf16)
    zero = jnp.zeros((16, LANES), bf16)
    wide = duos * 2 * LOW
    lane_at = lax.broadcasted_iota(jnp.int32, (16, wide), 1)
    lane_pair = lane_at // (2 * LOW) * 2 + lane_at // HIGH % 2
    depth = math.gcd(rows, DEPTH)

    def one_group(dest, g):
        total = None
        for step in range(rows // depth):
            tops = []
            lows = []
            for d in range(duos):
                c = dest * share + d % share
                p = g * (duos // share * 2 * classes) + dest * share + (d // share * 2 * classes + d % share)
                top = [[], []]
                hot = [[] for _ in ids]
                for t in range(step * depth // LANES, (step + 1) * depth // LANES):

                    def both(ref):
                        a = ref[t, pl.ds(p, 8, stride=0), :]
                        b = ref[t, pl.ds(p + classes, 8, stride=0), :]
                        return jnp.concatenate([a, b], axis=0).astype(bf16)

                    lo = both(low)
                    hi = both(high)
                    g_row = grad_rows[c, t]
                    h_row = hess_rows[c, t]
                    for n, i in enumerate(ids):
                        hot[n].append(jnp.where(lo == i, one, zero))
                    same = hi == ids[0]
                    top[0].append(jnp.where(same, g_row, zero))
                    top[1].append(jnp.where(same, h_row, zero))
                for n in range(0, len(ids), 2):
                    lows.append(jnp.concatenate([
                        jnp.concatenate(pair, axis=0).astype(narrow) for pair in zip(hot[n], hot[n + 1])
                    ], axis=1))
                tops += [jnp.concatenate(r, axis=1) for r in top]
            product = lax.dot_general(
                jnp.concatenate(tops, axis=0), jnp.concatenate(lows, axis=0), NT, preferred_element_type=f32
            )
            total = product if total is None else total + product
        kept = None
        for d in range(duos):
            for s in range(2):
                at = d * 32 + s * 8
                piece = jnp.concatenate([total[at : at + 8], total[at + 16 : at + 24]], axis=0)
                kept = piece if kept is None else jnp.where(lane_pair == 2 * d + s, piece, kept)
        return kept

    def each_dest(j, carry):
        def some(i, inner):
            for u in range(unroll):
                at = (j * groups_each) + i * unroll + u
                k = at // groups_each
                dest = 2 * lax.rem(chip + k // 2 + 1, chips) + lax.rem(core + 1 + lax.rem(k, 2), 2)
                g = lax.rem(at, groups_each)
                work[k, g] = one_group(dest, g)
            return inner

        lax.fori_loop(0, groups_each // unroll, some, 0)
        s = j // 2
        own = lax.rem(j, 2)

        def pass_on(n):
            one_copy(n).wait_recv()
            work[2 * n + 1] = work[2 * n + 1] + first[n]
            two_copy(n).start()

        @pl.when(j == 1)
        def _():
            with jax.named_scope("rowbarrier"):
                pl.semaphore_wait(barrier, n_row - 1)
            for k in range(1, n_row):
                sum_copy(k).start()
            one_copy(0).start()

        @pl.when((own == 0) & (j > 1))
        def _():
            one_copy(s).start()

        @pl.when(j == 3)
        def _():
            pass_on(0)

        @pl.when((own == 1) & (s > 0) & (s < chips - 1))
        def _():
            pass_on(s)

        return carry

    with jax.named_scope("hist"):
        lax.fori_loop(0, 2 * chips, each_dest, 0)

    load.wait()
    total = sums[0]
    with jax.named_scope("sumwait"):
        for k in range(1, n_row):
            sum_copy(k).wait()
    for k in range(1, n_row):
        total = total + sums[k]
    grad_left = total[:, 0:1]
    hess_left = total[:, 1:2]
    left_leaf = -grad_left / (hess_left + reg_lambda)
    right_leaf = -(total[:, 2:3] - grad_left) / (total[:, 3:4] - hess_left + reg_lambda)
    for b in range(blocks):
        cols = slice(b * block, (b + 1) * block)
        new_ref[:, cols] = x_ref[:, cols] + step_rate * jnp.where(left[:, cols] > 0.5, left_leaf, right_leaf)

    with jax.named_scope("tailwait"):
        one_copy(chips - 1).wait_recv()
        for s in range(chips):
            one_copy(s).wait_send()
        for s in range(chips - 1):
            two_copy(s).wait()
    summed = work[2 * chips - 1] + first[chips - 1]
    for s in range(chips - 1):
        summed = summed + second[s]
    count = groups_each * 2 * HIGH
    here = summed.reshape(count, wide)
    a = lax.broadcasted_iota(jnp.int32, (wide, 2 * wide), 0)
    b = lax.broadcasted_iota(jnp.int32, (wide, 2 * wide), 1)
    duo = a // (2 * LOW)
    pair = (duo // share * 2 + a // HIGH % 2) * share + duo % share
    value = a // (2 * HIGH) % (LOW // HIGH) * HIGH + a % HIGH
    target = b % wide
    keep = (pair == target // LOW) & ((b >= wide) | (value <= target % LOW))
    pieces = []
    rest = here
    for _ in range(3):
        piece = rest.astype(bf16)
        pieces.append(piece)
        rest = rest - piece.astype(f32)
    spread = lax.dot_general(
        jnp.concatenate(pieces, axis=0), keep.astype(f32).astype(bf16), (((1,), (0,)), ((), ())),
        preferred_element_type=f32,
    )
    spread = spread[:count] + spread[count : 2 * count] + spread[2 * count :]
    level = lax.broadcasted_iota(jnp.int32, (HIGH, wide), 0)

    def running(top):
        inside = spread[top : top + HIGH, :wide]
        upto = spread[top : top + HIGH, wide:]
        for shift in (1, 2, 4):
            upto = upto + jnp.where(level >= shift, pltpu.roll(upto, shift, 0), 0.0)
        before = jnp.where(level >= 1, pltpu.roll(upto, 1, 0), 0.0)
        return inside + before, upto[HIGH - 1 :]

    row_at = lax.broadcasted_iota(jnp.int32, (HIGH, BINS), 0)
    block_at = lax.broadcasted_iota(jnp.int32, (HIGH, BINS), 1) // LOW
    for g in range(groups_each):
        gl, ga = running(g * 2 * HIGH)
        hl, ha = running(g * 2 * HIGH + HIGH)
        gains = (
            gl * gl / (hl + reg_lambda)
            + (ga - gl) * (ga - gl) / (ha - hl + reg_lambda)
            - ga * ga / (ha + reg_lambda)
        )
        if wide < BINS:
            gains = jnp.concatenate([gains, jnp.zeros((HIGH, BINS - wide), f32)], axis=1)
        turned = gains
        for d in range(1, HIGH):
            moved = pltpu.roll(pltpu.roll(gains, HIGH - d, 0), LOW * d, 1)
            turned = jnp.where((row_at + d) % HIGH == block_at, moved, turned)
        each = 2 * duos // share
        for k in range(each):
            gains_ref[g * each + k] = turned[k * share : (k + 1) * share]


def deliver(new_ref, gains_ref, new_hbm, gains_hbm, sem):
    copies = [
        pltpu.make_async_copy(new_ref, new_hbm, sem.at[0]),
        pltpu.make_async_copy(gains_ref, gains_hbm, sem.at[1]),
    ]
    for copy in copies:
        copy.start()
    for copy in copies:
        copy.wait()


def local(n_cls, n_row, binned, labels, logits, elected, split_slot, split_bin):
    rows, classes = logits.shape
    columns = binned.shape[1]
    features = elected.shape[1]
    pairs = classes * features
    share = classes // n_row
    duos = math.gcd(share * features // 2, 4)
    groups_each = share * features // 2 // duos
    unroll = math.gcd(groups_each, UNROLL)
    chips = n_row // 2
    blocks = rows // math.gcd(rows, BLOCK)
    halves = math.gcd(blocks, 2)
    tiles = rows // LANES
    dma = pltpu.SemaphoreType.DMA
    part = (chips, groups_each, 2 * HIGH, duos * 2 * LOW)
    anywhere = pl.BlockSpec(memory_space=pltpu.HBM)
    vmem = pltpu.VMEM

    inside = pl.BlockSpec(memory_space=pltpu.VMEM)
    logits_t = pltpu.with_memory_space_constraint(logits.T, pltpu.HBM)
    made = pl.pallas_call(
        functools.partial(prepare, n_cls),
        out_shape=[
            jax.ShapeDtypeStruct((tiles, pairs, LANES), f32), jax.ShapeDtypeStruct((tiles, pairs, LANES), f32),
            jax.ShapeDtypeStruct((classes, rows), f32),
            jax.ShapeDtypeStruct((classes, tiles, 16, LANES), bf16),
            jax.ShapeDtypeStruct((classes, tiles, 16, LANES), bf16),
            jax.ShapeDtypeStruct((classes, LANES), f32),
        ],
        in_specs=[anywhere] * 6,
        out_specs=[inside] * 6,
        scratch_shapes=[
            vmem((rows, columns), jnp.int32), vmem((classes, rows), f32), vmem((1, rows), jnp.int32),
            vmem((features, classes), jnp.int32), vmem((1, classes), jnp.int32), vmem((1, classes), jnp.int32),
            vmem((128, 128), f32),
            vmem((pairs + classes, columns), bf16),
            vmem((tiles, classes, LANES), f32), vmem((tiles, classes, LANES), f32),
            vmem((halves, n_cls, 2, rows // halves), f32),
            dma((blocks + 5,)), dma((halves, n_cls)), dma((halves, n_cls)),
        ],
        compiler_params=pltpu.CompilerParams(
            vmem_limit_bytes=24 * 1024 * 1024, collective_id=0, has_side_effects=True,
        ),
        name="prepare",
    )(
        pltpu.with_memory_space_constraint(binned, pltpu.HBM), logits_t,
        *[pltpu.with_memory_space_constraint(array, pltpu.HBM) for array in (
            labels.reshape(1, rows), elected.T, split_slot.reshape(1, classes), split_bin.reshape(1, classes),
        )]
    )
    new, gains = pl.pallas_call(
        functools.partial(reduce, n_row, duos, groups_each, unroll, share, features),
        out_shape=[
            jax.ShapeDtypeStruct((classes, rows), f32), jax.ShapeDtypeStruct((features, share, BINS), f32),
        ],
        in_specs=[anywhere] + [inside] * 6,
        out_specs=[inside] * 2,
        scratch_shapes=[
            vmem((classes, rows), f32), vmem((n_row, classes, LANES), f32),
            vmem((2 * chips, *part[1:]), f32), vmem(part, f32), vmem(part, f32),
            dma((1,)), dma((n_row,)), dma((n_row,)),
            dma((chips,)), dma((chips,)), dma((chips,)), dma((chips,)),
        ],
        compiler_params=pltpu.CompilerParams(
            vmem_limit_bytes=24 * 1024 * 1024, collective_id=1, has_side_effects=True,
        ),
        name="reduce",
    )(logits_t, *[pltpu.with_memory_space_constraint(array, pltpu.VMEM) for array in made])
    new, gains = pl.pallas_call(
        deliver,
        out_shape=[jax.ShapeDtypeStruct(new.shape, f32), jax.ShapeDtypeStruct(gains.shape, f32)],
        in_specs=[inside] * 2,
        out_specs=[pl.BlockSpec(memory_space=pltpu.HBM)] * 2,
        scratch_shapes=[dma((2,))],
        name="deliver",
    )(*[pltpu.with_memory_space_constraint(array, pltpu.VMEM) for array in (new, gains)])
    return new.T, gains.transpose(1, 0, 2)


def solution(mesh):
    return jax.shard_map(
        functools.partial(local, mesh.shape["cls"], mesh.shape["row"]),
        mesh=mesh,
        in_specs=(P("row", None), P("row"), P("row", "cls"), P("cls", None), P("cls"), P("cls")),
        out_specs=(P("row", "cls"), P(("cls", "row"), None, None)),
        check_vma=False,
    )
```
